32 devices in a mesh: py: 8 (over z, x), px: 4 (over y, core).
Axes of the slice: x: 2, y: 2, z: 4, core: 2. Of those that a mesh axis runs over, the one named last changes fastest.
Arguments:
- density: float32 [256, 128, 128], P('py', 'px'), may hold values from 0.5 to 2
- conductance: float32 [256, 128, 128], P('py', 'px'), may hold values from 0.03 to 0.22
- source: float32 [256, 128, 128], P('py', 'px'), may hold values from -0.2 to 0.2
Outputs:
- anomaly: float32 [256, 128, 128], P('py', 'px')
- density_end: float32 [256, 128, 128], P('py', 'px')
The draws below stay inside these ranges and needn't reach their ends.
All inputs are finite; a program needn't handle non-finite values.
Results may differ from the reference program's by a relative error of at most 0.00002.
Values sent between devices are 32-bit elements; how exact they have to be, the bound alone decides.
A program may use at most 64 MiB of HBM per device.

```python
import jax
import jax.numpy as jnp
from jax import lax

GRID_Y = 256
GRID_X = 128
LEVELS = 128
STEPS = 6


def steps_of(rng, shape, cuts, least, high):
    loudness, own = 1.0, jax.random.fold_in(rng, 6)
    for dim, shards_of in cuts:
        steps = jnp.exp(jax.random.uniform(jax.random.fold_in(own, dim), (shards_of,), jnp.float32, least / len(cuts), high / len(cuts)))
        loudness = loudness * jnp.repeat(steps, shape[dim] // shards_of).reshape([-1 if axis == dim else 1 for axis in range(len(shape))])
    return loudness


def setup_inputs(seed: int = 0) -> dict:
    key_list = jax.random.split(jax.random.key(seed), 4)
    return {
        "density": jnp.clip(0.5 + 1.5 * jax.random.uniform(key_list[0], (GRID_Y, GRID_X, LEVELS), jnp.float32) ** steps_of(key_list[0], (GRID_Y, GRID_X, LEVELS), ((0, 8), (1, 4)), -0.2, 0.2), 0.5, 2.0),
        "conductance": jnp.clip(0.03 + 0.19 * jax.random.uniform(key_list[1], (GRID_Y, GRID_X, LEVELS), jnp.float32) ** steps_of(key_list[1], (GRID_Y, GRID_X, LEVELS), ((0, 8), (1, 4)), -0.2, 0.2), 0.03, 0.22),
        "source": jnp.clip(jax.random.uniform(key_list[2], (GRID_Y, GRID_X, LEVELS), jnp.float32, -0.2, 0.2) * steps_of(key_list[2], (GRID_Y, GRID_X, LEVELS), ((0, 8), (1, 4)), -0.4, 0.0), -0.2, 0.2),
    }


def strip_edges(values, dims):
    for dim in dims:
        values = lax.slice_in_dim(values, 1, values.shape[dim] - 1, axis=dim)
    return values

def neighbour(values, dim, start, dims):
    others = [other for other in dims if other != dim]
    values = strip_edges(values, others)
    return lax.slice_in_dim(values, start, start + values.shape[dim] - 2, axis=dim)

def one_step(padded, conductance, source):
    middle = strip_edges(padded, (0, 1))
    lower = [neighbour(padded, dim, 0, (0, 1)) for dim in (0, 1)]
    upper = [neighbour(padded, dim, 2, (0, 1)) for dim in (0, 1)]
    spread = lower[0] + upper[0] + lower[1] + upper[1] - 4.0 * middle
    return middle + conductance * spread + source

def reference(density, conductance, source):
    for step in range(STEPS):
        density = one_step(jnp.pad(density, ((1, 1), (1, 1), (0, 0)), mode='constant'), conductance, source)
    line_mean = lax.optimization_barrier(jnp.mean(density, axis=0, keepdims=True))
    centred = density - line_mean
    line_variance = lax.optimization_barrier(jnp.mean(centred * centred, axis=0, keepdims=True))
    anomaly = centred * lax.rsqrt(line_variance + 0.0001)
    return (anomaly, density)
```

```python
import functools

import jax
import jax.numpy as jnp
from jax import lax
from jax.experimental import pallas as pl
from jax.experimental.pallas import tpu as pltpu
from jax.sharding import PartitionSpec as P

ROUNDS = (3, 3)
DEEP = max(ROUNDS)
PAD = 4
DIRECTIONS = [(0, -1), (0, 1), (-1, 0), (1, 0), (-1, -1), (-1, 1), (1, -1), (1, 1)]
MESH = pl.DeviceIdType.MESH


def edge(direction, size, depth, own):
    if direction < 0:
        return (own, depth), (own + size, depth)
    if direction > 0:
        return (own + size - depth, depth), (own - depth, depth)
    return (own, size), (own, size)


def kernel(py, px, field, conductance, source, density_out, mean_out, scale_out,
           padded, work, coefficients, stats, local_sem, send_sem, recv_sem, stat_send, stat_recv):
    rows, columns, levels = field.shape
    width = columns + 2 * PAD
    my, mx = lax.axis_index("py"), lax.axis_index("px")

    def exists(dy, dx):
        here = jnp.bool_(True)
        if dy:
            here = here & ((my > 0) if dy < 0 else (my < py - 1))
        if dx:
            here = here & ((mx > 0) if dx < 0 else (mx < px - 1))
        return here

    inner = (pl.ds(DEEP, rows), pl.ds(PAD, columns))
    loads = []
    for i, (src, dst) in enumerate(
        [(field, padded.at[0]), (conductance, coefficients.at[0]), (source, coefficients.at[1])]
    ):
        loads.append(pltpu.make_async_copy(src, dst.at[inner], local_sem.at[i]))
        loads[-1].start()

    barrier = pltpu.get_barrier_semaphore()
    expected = jnp.int32(py - 1)
    for step in range(1, py):
        pl.semaphore_signal(barrier, 1, device_id=(lax.rem(my + step, py), mx), device_id_type=MESH)
    for dy, dx in DIRECTIONS:
        if dx:
            there = exists(dy, dx)
            expected = expected + there.astype(jnp.int32)

            @pl.when(there)
            def _():
                pl.semaphore_signal(barrier, 1, device_id=(my + dy, mx + dx), device_id_type=MESH)

    holders = [padded.at[r] for r in range(len(ROUNDS))] + [coefficients.at[0], coefficients.at[1]]
    for dim, direction in ((0, -1), (0, 1), (1, -1), (1, 1)):
        outside = ~exists(*((direction, 0) if dim == 0 else (0, direction)))

        @pl.when(outside)
        def _():
            for holder in holders:
                if dim == 0:
                    start = 0 if direction < 0 else DEEP + rows
                    holder[pl.ds(start, DEEP)] = jnp.zeros((DEEP, width, levels), jnp.float32)
                else:
                    start = 0 if direction < 0 else PAD + columns
                    holder[:, pl.ds(start, PAD)] = jnp.zeros((rows + 2 * DEEP, PAD, levels), jnp.float32)

    pl.semaphore_wait(barrier, expected)

    def exchange(number, arrays):
        for d, (dy, dx) in enumerate(DIRECTIONS):
            copies = []
            for a, (src, row0, column0, dst, depth) in enumerate(arrays):
                reach = depth - 1 if dy and dx else depth
                if reach < 1:
                    continue
                (y_from, y_size), _ = edge(dy, rows, reach, row0)
                (x_from, x_size), _ = edge(dx, columns, reach, column0)
                _, (y_to, _) = edge(dy, rows, reach, DEEP)
                _, (x_to, _) = edge(dx, columns, reach, PAD)
                copies.append(
                    pltpu.make_async_remote_copy(
                        src_ref=src.at[pl.ds(y_from, y_size), pl.ds(x_from, x_size)],
                        dst_ref=dst.at[pl.ds(y_to, y_size), pl.ds(x_to, x_size)],
                        send_sem=send_sem.at[number, a, d],
                        recv_sem=recv_sem.at[number, a, d],
                        device_id=(my + dy, mx + dx),
                        device_id_type=MESH,
                    )
                )
            yield (dy, dx), copies

    def start(copies):
        for (dy, dx), group in copies:
            @pl.when(exists(dy, dx))
            def _():
                for copy in group:
                    copy.start()

    def wait_recv(copies):
        for (dy, dx), group in copies:
            @pl.when(exists(-dy, -dx))
            def _():
                for copy in group:
                    copy.wait_recv()

    def wait_send(copies):
        for (dy, dx), group in copies:
            @pl.when(exists(dy, dx))
            def _():
                for copy in group:
                    copy.wait_send()

    tall = rows + 2 * DEEP
    flat_conductance = coefficients.at[0].reshape(tall * width, levels)
    flat_source = coefficients.at[1].reshape(tall * width, levels)

    def advance(old, first, count, column, wide, put, carry):
        flat = old.reshape(tall * width, levels)

        def row(i, state):
            above, middle, carry = state
            at = (first + i) * width + column
            below = flat[pl.ds(at + width, wide), :]
            sides = flat[pl.ds(at - 1, wide), :] + flat[pl.ds(at + 1, wide), :]
            spread = (above + below) + sides - 4.0 * middle
            later = middle + flat_conductance[pl.ds(at, wide), :] * spread + flat_source[pl.ds(at, wide), :]
            return middle, below, put(i, later, carry)

        at = first * width + column
        state = (flat[pl.ds(at - width, wide), :], flat[pl.ds(at, wide), :], carry)
        return lax.fori_loop(0, count, row, state, unroll=2)[2]

    total = jnp.zeros((columns, levels), jnp.float32)
    waiting = []
    for number, steps in enumerate(ROUNDS):
        if number == 0:
            arrays = [
                (field, 0, 0, padded.at[0], steps),
                (conductance, 0, 0, coefficients.at[0], DEEP - 1),
                (source, 0, 0, coefficients.at[1], DEEP - 1),
            ]
        else:
            arrays = [(padded.at[number], DEEP, PAD, padded.at[number], steps)]
        copies = list(exchange(number, arrays))
        start(copies)
        if number == 0:
            for copy in loads:
                copy.wait()
        wait_recv(copies)
        waiting.append(copies)
        old = padded.at[number]
        for step in range(steps):
            margin = steps - 1 - step
            if margin:
                new = work.at[step % 2]
                flat_new = new.reshape(tall * width, levels)
                first = DEEP - margin

                def put(i, later, carry, first=first, flat_new=flat_new):
                    flat_new[pl.ds((first + i) * width, width), :] = later
                    return carry

                advance(old, first, rows + 2 * margin, 0, width, put, 0)
                old = new
            elif number < len(ROUNDS) - 1:
                flat_new = padded.at[number + 1].reshape(tall * width, levels)

                def put(i, later, carry, flat_new=flat_new):
                    flat_new[pl.ds((DEEP + i) * width + PAD, columns), :] = later
                    return carry

                advance(old, DEEP, rows, PAD, columns, put, 0)
            else:

                def put(i, later, carry):
                    density_out[i] = later
                    return carry + later

                total = advance(old, DEEP, rows, PAD, columns, put, total)

    local_mean = total * (1.0 / rows)

    def square(i, carry):
        away = density_out[i] - local_mean
        return carry + away * away

    squares = lax.fori_loop(0, rows, square, jnp.zeros((columns, levels), jnp.float32), unroll=4)
    stats[0, 0] = local_mean
    stats[0, 1] = squares
    order = sorted(range(1, py), key=lambda step: -min(step, py - step))
    sums = []
    for step in order:
        copy = pltpu.make_async_remote_copy(
            src_ref=stats.at[0],
            dst_ref=stats.at[step],
            send_sem=stat_send.at[step],
            recv_sem=stat_recv.at[step],
            device_id=(lax.rem(my + step, py), mx),
            device_id_type=MESH,
        )
        copy.start()
        sums.append(copy)
    for copies in waiting:
        wait_send(copies)
    for copy in sums:
        copy.wait_recv()
    mean = stats[0, 0]
    for step in range(1, py):
        mean = mean + stats[step, 0]
    mean = mean * (1.0 / py)
    inside = stats[0, 1]
    between = (stats[0, 0] - mean) * (stats[0, 0] - mean)
    for step in range(1, py):
        inside = inside + stats[step, 1]
        between = between + (stats[step, 0] - mean) * (stats[step, 0] - mean)
    variance = inside * (1.0 / (rows * py)) + between * (1.0 / py)
    mean_out[...] = mean
    scale_out[...] = lax.rsqrt(variance + 0.0001)
    for copy in sums:
        copy.wait_send()


def per_device(py, px, density, conductance, source):
    rows, columns, levels = density.shape
    tall, width = rows + 2 * DEEP, columns + 2 * PAD
    vmem = pl.BlockSpec(memory_space=pltpu.VMEM)
    line = jax.ShapeDtypeStruct((columns, levels), jnp.float32)
    density, mean, scale = pl.pallas_call(
        functools.partial(kernel, py, px),
        out_shape=[jax.ShapeDtypeStruct(density.shape, jnp.float32), line, line],
        in_specs=[pl.BlockSpec(memory_space=pl.ANY)] * 3,
        out_specs=[vmem] * 3,
        scratch_shapes=[
            pltpu.VMEM((len(ROUNDS), tall, width, levels), jnp.float32),
            pltpu.VMEM((2, tall, width, levels), jnp.float32),
            pltpu.VMEM((2, tall, width, levels), jnp.float32),
            pltpu.VMEM((py, 2, columns, levels), jnp.float32),
            pltpu.SemaphoreType.DMA((3,)),
            pltpu.SemaphoreType.DMA((len(ROUNDS), 3, len(DIRECTIONS))),
            pltpu.SemaphoreType.DMA((len(ROUNDS), 3, len(DIRECTIONS))),
            pltpu.SemaphoreType.DMA((py,)),
            pltpu.SemaphoreType.DMA((py,)),
        ],
        compiler_params=pltpu.CompilerParams(collective_id=0, has_side_effects=True),
    )(density, conductance, source)
    return (density - mean) * scale, density


def solution(mesh):
    spec = P("py", "px", None)
    return jax.shard_map(
        functools.partial(per_device, mesh.shape["py"], mesh.shape["px"]),
        mesh=mesh, in_specs=(spec,) * 3, out_specs=(spec,) * 2, check_vma=False,
    )
```

```python
import functools

import jax
import jax.numpy as jnp
from jax import lax
from jax.experimental import pallas as pl
from jax.experimental.pallas import tpu as pltpu
from jax.sharding import PartitionSpec as P

ROUNDS = (3, 3)
DEEP = max(ROUNDS)
PAD = 4
DIRECTIONS = [(0, -1), (0, 1), (-1, 0), (1, 0), (-1, -1), (-1, 1), (1, -1), (1, 1)]
MESH = pl.DeviceIdType.MESH


def edge(direction, size, depth, own):
    if direction < 0:
        return (own, depth), (own + size, depth)
    if direction > 0:
        return (own + size - depth, depth), (own - depth, depth)
    return (own, size), (own, size)


def kernel(py, px, field, conductance, source, density_out, mean_out, scale_out,
           padded, work, coefficients, stats, local_sem, send_sem, recv_sem, stat_send, stat_recv):
    rows, columns, levels = field.shape
    width = columns + 2 * PAD
    my, mx = lax.axis_index("py"), lax.axis_index("px")

    def exists(dy, dx):
        here = jnp.bool_(True)
        if dy:
            here = here & ((my > 0) if dy < 0 else (my < py - 1))
        if dx:
            here = here & ((mx > 0) if dx < 0 else (mx < px - 1))
        return here

    inner = (pl.ds(DEEP, rows), pl.ds(PAD, columns))
    loads = []
    for i, (src, dst) in enumerate(
        [(field, padded.at[0]), (conductance, coefficients.at[0]), (source, coefficients.at[1])]
    ):
        loads.append(pltpu.make_async_copy(src, dst.at[inner], local_sem.at[i]))
        loads[-1].start()

    barrier = pltpu.get_barrier_semaphore()
    expected = jnp.int32(py - 1)
    for step in range(1, py):
        pl.semaphore_signal(barrier, 1, device_id=(lax.rem(my + step, py), mx), device_id_type=MESH)
    for dy, dx in DIRECTIONS:
        if dx:
            there = exists(dy, dx)
            expected = expected + there.astype(jnp.int32)

            @pl.when(there)
            def _():
                pl.semaphore_signal(barrier, 1, device_id=(my + dy, mx + dx), device_id_type=MESH)

    holders = [padded.at[r] for r in range(len(ROUNDS))] + [coefficients.at[0], coefficients.at[1]]
    for dim, direction in ((0, -1), (0, 1), (1, -1), (1, 1)):
        outside = ~exists(*((direction, 0) if dim == 0 else (0, direction)))

        @pl.when(outside)
        def _():
            for holder in holders:
                if dim == 0:
                    start = 0 if direction < 0 else DEEP + rows
                    holder[pl.ds(start, DEEP)] = jnp.zeros((DEEP, width, levels), jnp.float32)
                else:
                    start = 0 if direction < 0 else PAD + columns
                    holder[:, pl.ds(start, PAD)] = jnp.zeros((rows + 2 * DEEP, PAD, levels), jnp.float32)

    pl.semaphore_wait(barrier, expected)

    def exchange(number, arrays):
        for d, (dy, dx) in enumerate(DIRECTIONS):
            copies = []
            for a, (src, row0, column0, dst, depth) in enumerate(arrays):
                reach = depth - 1 if dy and dx else depth
                if reach < 1:
                    continue
                (y_from, y_size), _ = edge(dy, rows, reach, row0)
                (x_from, x_size), _ = edge(dx, columns, reach, column0)
                _, (y_to, _) = edge(dy, rows, reach, DEEP)
                _, (x_to, _) = edge(dx, columns, reach, PAD)
                copies.append(
                    pltpu.make_async_remote_copy(
                        src_ref=src.at[pl.ds(y_from, y_size), pl.ds(x_from, x_size)],
                        dst_ref=dst.at[pl.ds(y_to, y_size), pl.ds(x_to, x_size)],
                        send_sem=send_sem.at[number, a, d],
                        recv_sem=recv_sem.at[number, a, d],
                        device_id=(my + dy, mx + dx),
                        device_id_type=MESH,
                    )
                )
            yield (dy, dx), copies

    def start(copies):
        for (dy, dx), group in copies:
            @pl.when(exists(dy, dx))
            def _():
                for copy in group:
                    copy.start()

    def wait_recv(copies):
        for (dy, dx), group in copies:
            @pl.when(exists(-dy, -dx))
            def _():
                for copy in group:
                    copy.wait_recv()

    def wait_send(copies):
        for (dy, dx), group in copies:
            @pl.when(exists(dy, dx))
            def _():
                for copy in group:
                    copy.wait_send()

    tall = rows + 2 * DEEP
    flat_conductance = coefficients.at[0].reshape(tall * width, levels)
    flat_source = coefficients.at[1].reshape(tall * width, levels)

    def advance(old, first, count, column, wide, put, carry):
        flat = old.reshape(tall * width, levels)

        def row(i, state):
            above, middle, carry = state
            at = (first + i) * width + column
            below = flat[pl.ds(at + width, wide), :]
            sides = flat[pl.ds(at - 1, wide), :] + flat[pl.ds(at + 1, wide), :]
            spread = (above + below) + sides - 4.0 * middle
            later = middle + flat_conductance[pl.ds(at, wide), :] * spread + flat_source[pl.ds(at, wide), :]
            return middle, below, put(i, later, carry)

        at = first * width + column
        state = (flat[pl.ds(at - width, wide), :], flat[pl.ds(at, wide), :], carry)
        return lax.fori_loop(0, count, row, state, unroll=2)[2]

    total = jnp.zeros((columns, levels), jnp.float32)
    waiting = []
    for number, steps in enumerate(ROUNDS):
        if number == 0:
            arrays = [
                (padded.at[0], DEEP, PAD, padded.at[0], steps),
                (coefficients.at[0], DEEP, PAD, coefficients.at[0], DEEP - 1),
                (coefficients.at[1], DEEP, PAD, coefficients.at[1], DEEP - 1),
            ]
        else:
            arrays = [(padded.at[number], DEEP, PAD, padded.at[number], steps)]
        copies = list(exchange(number, arrays))
        if number == 0:
            for copy in loads:
                copy.wait()
        start(copies)
        wait_recv(copies)
        waiting.append(copies)
        old = padded.at[number]
        for step in range(steps):
            margin = steps - 1 - step
            if margin:
                new = work.at[step % 2]
                flat_new = new.reshape(tall * width, levels)
                first = DEEP - margin

                def put(i, later, carry, first=first, flat_new=flat_new):
                    flat_new[pl.ds((first + i) * width, width), :] = later
                    return carry

                advance(old, first, rows + 2 * margin, 0, width, put, 0)
                old = new
            elif number < len(ROUNDS) - 1:
                flat_new = padded.at[number + 1].reshape(tall * width, levels)

                def put(i, later, carry, flat_new=flat_new):
                    flat_new[pl.ds((DEEP + i) * width + PAD, columns), :] = later
                    return carry

                advance(old, DEEP, rows, PAD, columns, put, 0)
            else:

                def put(i, later, carry):
                    density_out[i] = later
                    return carry + later

                total = advance(old, DEEP, rows, PAD, columns, put, total)

    local_mean = total * (1.0 / rows)

    def square(i, carry):
        away = density_out[i] - local_mean
        return carry + away * away

    squares = lax.fori_loop(0, rows, square, jnp.zeros((columns, levels), jnp.float32), unroll=4)
    stats[0, 0] = local_mean
    stats[0, 1] = squares
    order = sorted(range(1, py), key=lambda step: -min(step, py - step))
    sums = []
    for step in order:
        copy = pltpu.make_async_remote_copy(
            src_ref=stats.at[0],
            dst_ref=stats.at[step],
            send_sem=stat_send.at[step],
            recv_sem=stat_recv.at[step],
            device_id=(lax.rem(my + step, py), mx),
            device_id_type=MESH,
        )
        copy.start()
        sums.append(copy)
    for copies in waiting:
        wait_send(copies)
    for copy in sums:
        copy.wait_recv()
    mean = stats[0, 0]
    for step in range(1, py):
        mean = mean + stats[step, 0]
    mean = mean * (1.0 / py)
    inside = stats[0, 1]
    between = (stats[0, 0] - mean) * (stats[0, 0] - mean)
    for step in range(1, py):
        inside = inside + stats[step, 1]
        between = between + (stats[step, 0] - mean) * (stats[step, 0] - mean)
    variance = inside * (1.0 / (rows * py)) + between * (1.0 / py)
    mean_out[...] = mean
    scale_out[...] = lax.rsqrt(variance + 0.0001)
    for copy in sums:
        copy.wait_send()

CHUNKS = 4


def finish(density, mean, scale, anomaly_out, density_out, anomaly, sem):
    rows = density.shape[0]
    whole = pltpu.make_async_copy(density, density_out, sem.at[CHUNKS])
    whole.start()
    part = rows // CHUNKS
    copies = []
    for chunk in range(CHUNKS):
        for i in range(chunk * part, (chunk + 1) * part):
            anomaly[i] = (density[i] - mean[...]) * scale[...]
        own = pl.ds(chunk * part, part)
        copies.append(pltpu.make_async_copy(anomaly.at[own], anomaly_out.at[own], sem.at[chunk]))
        copies[-1].start()
    for copy in copies:
        copy.wait()
    whole.wait()


def per_device(py, px, density, conductance, source):
    rows, columns, levels = density.shape
    tall, width = rows + 2 * DEEP, columns + 2 * PAD
    vmem = pl.BlockSpec(memory_space=pltpu.VMEM)
    line = jax.ShapeDtypeStruct((columns, levels), jnp.float32)
    density, conductance, source = (pltpu.with_memory_space_constraint(x, pltpu.HBM) for x in (density, conductance, source))
    density, mean, scale = pl.pallas_call(
        functools.partial(kernel, py, px),
        out_shape=[jax.ShapeDtypeStruct(density.shape, jnp.float32), line, line],
        in_specs=[pl.BlockSpec(memory_space=pltpu.HBM)] * 3,
        out_specs=[vmem] * 3,
        scratch_shapes=[
            pltpu.VMEM((len(ROUNDS), tall, width, levels), jnp.float32),
            pltpu.VMEM((2, tall, width, levels), jnp.float32),
            pltpu.VMEM((2, tall, width, levels), jnp.float32),
            pltpu.VMEM((py, 2, columns, levels), jnp.float32),
            pltpu.SemaphoreType.DMA((3,)),
            pltpu.SemaphoreType.DMA((len(ROUNDS), 3, len(DIRECTIONS))),
            pltpu.SemaphoreType.DMA((len(ROUNDS), 3, len(DIRECTIONS))),
            pltpu.SemaphoreType.DMA((py,)),
            pltpu.SemaphoreType.DMA((py,)),
        ],
        compiler_params=pltpu.CompilerParams(collective_id=0, has_side_effects=True, vmem_limit_bytes=10*2**20),
    )(density, conductance, source)
    return pl.pallas_call(
        finish,
        out_shape=[jax.ShapeDtypeStruct(density.shape, jnp.float32)] * 2,
        in_specs=[vmem] * 3,
        out_specs=[pl.BlockSpec(memory_space=pltpu.HBM)] * 2,
        scratch_shapes=[pltpu.VMEM(density.shape, jnp.float32), pltpu.SemaphoreType.DMA((CHUNKS + 1,))],
        compiler_params=pltpu.CompilerParams(vmem_limit_bytes=4 * 2**20),
    )(density, mean, scale)


def solution(mesh):
    spec = P("py", "px", None)
    return jax.shard_map(
        functools.partial(per_device, mesh.shape["py"], mesh.shape["px"]),
        mesh=mesh, in_specs=(spec,) * 3, out_specs=(spec,) * 2, check_vma=False,
    )
```

```python
import functools

import jax
import jax.numpy as jnp
from jax import lax
from jax.experimental import pallas as pl
from jax.experimental.pallas import tpu as pltpu
from jax.sharding import PartitionSpec as P

ROUNDS = (3, 3)
DEEP = max(ROUNDS)
PAD = 4
DIRECTIONS = [(0, -1), (0, 1), (-1, 0), (1, 0), (-1, -1), (-1, 1), (1, -1), (1, 1)]
MESH = pl.DeviceIdType.MESH


def edge(direction, size, depth, own):
    if direction < 0:
        return (own, depth), (own + size, depth)
    if direction > 0:
        return (own + size - depth, depth), (own - depth, depth)
    return (own, size), (own, size)


def kernel(py, px, inner, field, conductance, source, density_out, mean_out, scale_out,
           padded, work, coefficients, stats, local_sem, send_sem, recv_sem, stat_send, stat_recv):
    rows, columns, levels = field.shape
    width = columns + 2 * PAD
    my, mx = lax.axis_index("py"), lax.axis_index("px")

    def exists(dy, dx):
        here = jnp.bool_(True)
        if dy:
            here = here & ((my > 0) if dy < 0 else (my < py - 1))
        if dx:
            here = here & ((mx > 0) if dx < 0 else (mx < px - 1))
        return here

    block = (pl.ds(DEEP, rows), pl.ds(PAD, columns))
    loads = []
    for i, (src, dst) in enumerate(
        [(field, padded.at[0]), (conductance, coefficients.at[0]), (source, coefficients.at[1])]
    ):
        loads.append(pltpu.make_async_copy(src, dst.at[block], local_sem.at[i]))
        loads[-1].start()

    barrier = pltpu.get_barrier_semaphore()
    expected = jnp.int32(py - 1)
    for step in range(1, py):
        pl.semaphore_signal(barrier, 1, device_id=(lax.rem(my + step, py), mx), device_id_type=MESH)
    for dy, dx in DIRECTIONS:
        if dx:
            there = exists(dy, dx)
            expected = expected + there.astype(jnp.int32)

            @pl.when(there)
            def _():
                pl.semaphore_signal(barrier, 1, device_id=(my + dy, mx + dx), device_id_type=MESH)

    holders = [padded.at[r] for r in range(len(ROUNDS))] + [coefficients.at[0], coefficients.at[1]]
    for dim, direction in ((0, -1), (0, 1), (1, -1), (1, 1)):
        outside = ~exists(*((direction, 0) if dim == 0 else (0, direction)))

        @pl.when(outside)
        def _():
            for holder in holders:
                if dim == 0:
                    start = 0 if direction < 0 else DEEP + rows
                    holder[pl.ds(start, DEEP)] = jnp.zeros((DEEP, width, levels), jnp.float32)
                else:
                    start = 0 if direction < 0 else PAD + columns
                    holder[:, pl.ds(start, PAD)] = jnp.zeros((rows + 2 * DEEP, PAD, levels), jnp.float32)

    pl.semaphore_wait(barrier, expected)

    def exchange(number, arrays):
        for d, (dy, dx) in enumerate(DIRECTIONS):
            copies = []
            for a, (src, row0, column0, dst, depth) in enumerate(arrays):
                reach = depth - 1 if dy and dx else depth
                if reach < 1:
                    continue
                (y_from, y_size), _ = edge(dy, rows, reach, row0)
                (x_from, x_size), _ = edge(dx, columns, reach, column0)
                _, (y_to, _) = edge(dy, rows, reach, DEEP)
                _, (x_to, _) = edge(dx, columns, reach, PAD)
                copies.append(
                    pltpu.make_async_remote_copy(
                        src_ref=src.at[pl.ds(y_from, y_size), pl.ds(x_from, x_size)],
                        dst_ref=dst.at[pl.ds(y_to, y_size), pl.ds(x_to, x_size)],
                        send_sem=send_sem.at[number, a, d],
                        recv_sem=recv_sem.at[number, a, d],
                        device_id=(my + dy, mx + dx),
                        device_id_type=MESH,
                    )
                )
            yield (dy, dx), copies

    def start(copies):
        for (dy, dx), group in copies:
            @pl.when(exists(dy, dx))
            def _():
                for copy in group:
                    copy.start()

    def wait_recv(copies):
        for (dy, dx), group in copies:
            @pl.when(exists(-dy, -dx))
            def _():
                for copy in group:
                    copy.wait_recv()

    def wait_send(copies):
        for (dy, dx), group in copies:
            @pl.when(exists(dy, dx))
            def _():
                for copy in group:
                    copy.wait_send()

    tall = rows + 2 * DEEP
    flat_conductance = coefficients.at[0].reshape(tall * width, levels)
    flat_source = coefficients.at[1].reshape(tall * width, levels)

    def advance(old, first, count, column, wide, put, carry):
        flat = old.reshape(tall * width, levels)

        def row(i, state):
            above, middle, carry = state
            at = (first + i) * width + column
            below = flat[pl.ds(at + width, wide), :]
            sides = flat[pl.ds(at - 1, wide), :] + flat[pl.ds(at + 1, wide), :]
            spread = (above + below) + sides - 4.0 * middle
            later = middle + flat_conductance[pl.ds(at, wide), :] * spread + flat_source[pl.ds(at, wide), :]
            return middle, below, put(i, later, carry)

        at = first * width + column
        state = (flat[pl.ds(at - width, wide), :], flat[pl.ds(at, wide), :], carry)
        return lax.fori_loop(0, count, row, state, unroll=2)[2]

    total = jnp.zeros((columns, levels), jnp.float32)
    waiting = []
    for number, steps in enumerate(ROUNDS):
        if number == 0:
            arrays = [
                (padded.at[0], DEEP, PAD, padded.at[0], steps),
                (coefficients.at[0], DEEP, PAD, coefficients.at[0], DEEP - 1),
                (coefficients.at[1], DEEP, PAD, coefficients.at[1], DEEP - 1),
            ]
        else:
            arrays = [(padded.at[number], DEEP, PAD, padded.at[number], steps)]
        copies = list(exchange(number, arrays))
        if number == 0:
            for copy in loads:
                copy.wait()
        start(copies)
        wait_recv(copies)
        waiting.append(copies)
        old = padded.at[number]
        for step in range(steps):
            margin = steps - 1 - step
            if margin:
                new = work.at[step % 2]
                flat_new = new.reshape(tall * width, levels)
                first = DEEP - margin

                def put(i, later, carry, first=first, flat_new=flat_new):
                    flat_new[pl.ds((first + i) * width, width), :] = later
                    return carry

                advance(old, first, rows + 2 * margin, 0, width, put, 0)
                old = new
            elif number < len(ROUNDS) - 1:
                flat_new = padded.at[number + 1].reshape(tall * width, levels)

                def put(i, later, carry, flat_new=flat_new):
                    flat_new[pl.ds((DEEP + i) * width + PAD, columns), :] = later
                    return carry

                advance(old, DEEP, rows, PAD, columns, put, 0)
            else:

                def put(i, later, carry):
                    density_out[i] = later
                    return carry + later

                total = advance(old, DEEP, rows, PAD, columns, put, total)

    local_mean = total * (1.0 / rows)

    def square(i, carry):
        away = density_out[i] - local_mean
        return carry + away * away

    squares = lax.fori_loop(0, rows, square, jnp.zeros((columns, levels), jnp.float32), unroll=4)
    stats[0, 0] = local_mean
    stats[0, 1] = squares
    outer = py // inner
    far_first = sorted(
        ((do, di) for do in range(outer) for di in range(inner) if do or di),
        key=lambda place: -(min(place[0], outer - place[0]) + min(place[1], inner - place[1])),
    )
    sums = []
    for do, di in far_first:
        step = do * inner + di
        peer = lax.rem(my // inner + do, outer) * inner + lax.rem(lax.rem(my, inner) + di, inner)
        copy = pltpu.make_async_remote_copy(
            src_ref=stats.at[0],
            dst_ref=stats.at[step],
            send_sem=stat_send.at[step],
            recv_sem=stat_recv.at[step],
            device_id=(peer, mx),
            device_id_type=MESH,
        )
        copy.start()
        sums.append(copy)
    for copies in waiting:
        wait_send(copies)
    for copy in sums:
        copy.wait_recv()
    mean = stats[0, 0]
    for step in range(1, py):
        mean = mean + stats[step, 0]
    mean = mean * (1.0 / py)
    inside = stats[0, 1]
    between = (stats[0, 0] - mean) * (stats[0, 0] - mean)
    for step in range(1, py):
        inside = inside + stats[step, 1]
        between = between + (stats[step, 0] - mean) * (stats[step, 0] - mean)
    variance = inside * (1.0 / (rows * py)) + between * (1.0 / py)
    mean_out[...] = mean
    scale_out[...] = lax.rsqrt(variance + 0.0001)
    for copy in sums:
        copy.wait_send()

CHUNKS = 4


def finish(density, mean, scale, anomaly_out, density_out, anomaly, sem):
    rows = density.shape[0]
    whole = pltpu.make_async_copy(density, density_out, sem.at[CHUNKS])
    whole.start()
    part = rows // CHUNKS
    copies = []
    for chunk in range(CHUNKS):
        for i in range(chunk * part, (chunk + 1) * part):
            anomaly[i] = (density[i] - mean[...]) * scale[...]
        own = pl.ds(chunk * part, part)
        copies.append(pltpu.make_async_copy(anomaly.at[own], anomaly_out.at[own], sem.at[chunk]))
        copies[-1].start()
    for copy in copies:
        copy.wait()
    whole.wait()


def per_device(py, px, inner, density, conductance, source):
    rows, columns, levels = density.shape
    tall, width = rows + 2 * DEEP, columns + 2 * PAD
    vmem = pl.BlockSpec(memory_space=pltpu.VMEM)
    line = jax.ShapeDtypeStruct((columns, levels), jnp.float32)
    density, conductance, source = (pltpu.with_memory_space_constraint(x, pltpu.HBM) for x in (density, conductance, source))
    density, mean, scale = pl.pallas_call(
        functools.partial(kernel, py, px, inner),
        out_shape=[jax.ShapeDtypeStruct(density.shape, jnp.float32), line, line],
        in_specs=[pl.BlockSpec(memory_space=pltpu.HBM)] * 3,
        out_specs=[vmem] * 3,
        scratch_shapes=[
            pltpu.VMEM((len(ROUNDS), tall, width, levels), jnp.float32),
            pltpu.VMEM((2, tall, width, levels), jnp.float32),
            pltpu.VMEM((2, tall, width, levels), jnp.float32),
            pltpu.VMEM((py, 2, columns, levels), jnp.float32),
            pltpu.SemaphoreType.DMA((3,)),
            pltpu.SemaphoreType.DMA((len(ROUNDS), 3, len(DIRECTIONS))),
            pltpu.SemaphoreType.DMA((len(ROUNDS), 3, len(DIRECTIONS))),
            pltpu.SemaphoreType.DMA((py,)),
            pltpu.SemaphoreType.DMA((py,)),
        ],
        compiler_params=pltpu.CompilerParams(collective_id=0, has_side_effects=True, vmem_limit_bytes=10*2**20),
    )(density, conductance, source)
    return pl.pallas_call(
        finish,
        out_shape=[jax.ShapeDtypeStruct(density.shape, jnp.float32)] * 2,
        in_specs=[vmem] * 3,
        out_specs=[pl.BlockSpec(memory_space=pltpu.HBM)] * 2,
        scratch_shapes=[pltpu.VMEM(density.shape, jnp.float32), pltpu.SemaphoreType.DMA((CHUNKS + 1,))],
        compiler_params=pltpu.CompilerParams(vmem_limit_bytes=4 * 2**20),
    )(density, mean, scale)


def solution(mesh):
    spec = P("py", "px", None)
    line = mesh.devices.reshape(mesh.shape["py"], -1)[:, 0] if mesh.axis_names[0] == "py" else []
    places = [getattr(device, "coords", (0, 0, 0))[2] for device in line]
    inner = max(1, places.count(places[0])) if places else 1
    return jax.shard_map(
        functools.partial(per_device, mesh.shape["py"], mesh.shape["px"], inner),
        mesh=mesh, in_specs=(spec,) * 3, out_specs=(spec,) * 2, check_vma=False,
    )
```

```python
import functools

import jax
import jax.numpy as jnp
from jax import lax
from jax.experimental import pallas as pl
from jax.experimental.pallas import tpu as pltpu
from jax.sharding import PartitionSpec as P

ROUNDS = (3, 3)
DEEP = max(ROUNDS)
PAD = 4
DIRECTIONS = [(-1, -1), (-1, 1), (1, -1), (1, 1), (-1, 0), (1, 0), (0, -1), (0, 1)]
MESH = pl.DeviceIdType.MESH


def edge(direction, size, depth, own):
    if direction < 0:
        return (own, depth), (own + size, depth)
    if direction > 0:
        return (own + size - depth, depth), (own - depth, depth)
    return (own, size), (own, size)


def kernel(py, px, inner, field, conductance, source, density_out, mean_out, scale_out,
           padded, work, coefficients, stats, local_sem, send_sem, recv_sem, stat_send, stat_recv):
    rows, columns, levels = field.shape
    width = columns + 2 * PAD
    my, mx = lax.axis_index("py"), lax.axis_index("px")

    def exists(dy, dx):
        here = jnp.bool_(True)
        if dy:
            here = here & ((my > 0) if dy < 0 else (my < py - 1))
        if dx:
            here = here & ((mx > 0) if dx < 0 else (mx < px - 1))
        return here

    block = (pl.ds(DEEP, rows), pl.ds(PAD, columns))
    loads = []
    for i, (src, dst) in enumerate(
        [(field, padded.at[0]), (conductance, coefficients.at[0]), (source, coefficients.at[1])]
    ):
        loads.append(pltpu.make_async_copy(src, dst.at[block], local_sem.at[i]))
        loads[-1].start()

    barrier = pltpu.get_barrier_semaphore()
    expected = jnp.int32(py - 1)
    for step in range(1, py):
        pl.semaphore_signal(barrier, 1, device_id=(lax.rem(my + step, py), mx), device_id_type=MESH)
    for dy, dx in DIRECTIONS:
        if dx:
            there = exists(dy, dx)
            expected = expected + there.astype(jnp.int32)

            @pl.when(there)
            def _():
                pl.semaphore_signal(barrier, 1, device_id=(my + dy, mx + dx), device_id_type=MESH)

    holders = [padded.at[r] for r in range(len(ROUNDS))] + [coefficients.at[0], coefficients.at[1]]
    for dim, direction in ((0, -1), (0, 1), (1, -1), (1, 1)):
        outside = ~exists(*((direction, 0) if dim == 0 else (0, direction)))

        @pl.when(outside)
        def _():
            for holder in holders:
                if dim == 0:
                    start = 0 if direction < 0 else DEEP + rows
                    holder[pl.ds(start, DEEP)] = jnp.zeros((DEEP, width, levels), jnp.float32)
                else:
                    start = 0 if direction < 0 else PAD + columns
                    holder[:, pl.ds(start, PAD)] = jnp.zeros((rows + 2 * DEEP, PAD, levels), jnp.float32)

    pl.semaphore_wait(barrier, expected)

    def exchange(number, arrays):
        for d, (dy, dx) in enumerate(DIRECTIONS):
            copies = []
            for a, (src, row0, column0, dst, depth) in enumerate(arrays):
                reach = depth - 1 if dy and dx else depth
                if reach < 1:
                    continue
                (y_from, y_size), _ = edge(dy, rows, reach, row0)
                (x_from, x_size), _ = edge(dx, columns, reach, column0)
                _, (y_to, _) = edge(dy, rows, reach, DEEP)
                _, (x_to, _) = edge(dx, columns, reach, PAD)
                copies.append(
                    pltpu.make_async_remote_copy(
                        src_ref=src.at[pl.ds(y_from, y_size), pl.ds(x_from, x_size)],
                        dst_ref=dst.at[pl.ds(y_to, y_size), pl.ds(x_to, x_size)],
                        send_sem=send_sem.at[number, a, d],
                        recv_sem=recv_sem.at[number, a, d],
                        device_id=(my + dy, mx + dx),
                        device_id_type=MESH,
                    )
                )
            yield (dy, dx), copies

    def start(copies):
        for (dy, dx), group in copies:
            @pl.when(exists(dy, dx))
            def _():
                for copy in group:
                    copy.start()

    def wait_recv(copies):
        for (dy, dx), group in copies:
            @pl.when(exists(-dy, -dx))
            def _():
                for copy in group:
                    copy.wait_recv()

    def wait_send(copies):
        for (dy, dx), group in copies:
            @pl.when(exists(dy, dx))
            def _():
                for copy in group:
                    copy.wait_send()

    tall = rows + 2 * DEEP
    flat_conductance = coefficients.at[0].reshape(tall * width, levels)
    flat_source = coefficients.at[1].reshape(tall * width, levels)

    def advance(old, first, count, column, wide, put, carry):
        flat = old.reshape(tall * width, levels)

        def row(i, state):
            above, middle, carry = state
            at = (first + i) * width + column
            below = flat[pl.ds(at + width, wide), :]
            sides = flat[pl.ds(at - 1, wide), :] + flat[pl.ds(at + 1, wide), :]
            spread = (above + below) + sides - 4.0 * middle
            later = middle + flat_conductance[pl.ds(at, wide), :] * spread + flat_source[pl.ds(at, wide), :]
            return middle, below, put(first - DEEP + i, later, carry)

        at = first * width + column
        state = (flat[pl.ds(at - width, wide), :], flat[pl.ds(at, wide), :], carry)
        return lax.fori_loop(0, count, row, state, unroll=min(count, 4))[2]

    total = jnp.zeros((columns, levels), jnp.float32)
    waiting = []
    for number, steps in enumerate(ROUNDS):
        if number == 0:
            arrays = [
                (padded.at[0], DEEP, PAD, padded.at[0], steps),
                (coefficients.at[0], DEEP, PAD, coefficients.at[0], DEEP - 1),
                (coefficients.at[1], DEEP, PAD, coefficients.at[1], DEEP - 1),
            ]
        else:
            arrays = [(padded.at[number], DEEP, PAD, padded.at[number], steps)]
        copies = list(exchange(number, arrays))
        if number == 0:
            for copy in loads:
                copy.wait()
        start(copies)
        waiting.append(copies)
        across = [copy for copy in copies if not copy[0][0]]
        wait_recv(across)
        for part in ("inside", "ends"):
            if part == "ends":
                wait_recv([copy for copy in copies if copy[0][0]])
            old = padded.at[number]
            for step in range(steps):
                margin = steps - 1 - step
                if part == "inside":
                    spans = [(DEEP + step + 1, rows - 2 * (step + 1))]
                else:
                    spans = [(DEEP - margin, steps), (DEEP + rows - step - 1, steps)]
                column, wide, new = PAD, columns, None
                if margin:
                    column, wide, new = 0, width, work.at[step]
                elif number < len(ROUNDS) - 1:
                    new = padded.at[number + 1]

                def put(i, later, carry, new=new, column=column, wide=wide):
                    if new is None:
                        density_out[i] = later
                        return carry + later
                    new.reshape(tall * width, levels)[pl.ds((DEEP + i) * width + column, wide), :] = later
                    return carry

                for first, count in spans:
                    total = advance(old, first, count, column, wide, put, total)
                old = new

    local_mean = total * (1.0 / rows)

    def square(i, carry):
        away = density_out[i] - local_mean
        return carry + away * away

    squares = lax.fori_loop(0, rows, square, jnp.zeros((columns, levels), jnp.float32), unroll=4)
    stats[0, 0] = local_mean
    stats[0, 1] = squares
    outer = py // inner
    far_first = sorted(
        ((do, di) for do in range(outer) for di in range(inner) if do or di),
        key=lambda place: -(min(place[0], outer - place[0]) + min(place[1], inner - place[1])),
    )
    sums = []
    for do, di in far_first:
        step = do * inner + di
        peer = lax.rem(my // inner + do, outer) * inner + lax.rem(lax.rem(my, inner) + di, inner)
        copy = pltpu.make_async_remote_copy(
            src_ref=stats.at[0],
            dst_ref=stats.at[step],
            send_sem=stat_send.at[step],
            recv_sem=stat_recv.at[step],
            device_id=(peer, mx),
            device_id_type=MESH,
        )
        copy.start()
        sums.append(copy)
    for copies in waiting:
        wait_send(copies)
    for copy in sums:
        copy.wait_recv()
    mean = stats[0, 0]
    for step in range(1, py):
        mean = mean + stats[step, 0]
    mean = mean * (1.0 / py)
    inside = stats[0, 1]
    between = (stats[0, 0] - mean) * (stats[0, 0] - mean)
    for step in range(1, py):
        inside = inside + stats[step, 1]
        between = between + (stats[step, 0] - mean) * (stats[step, 0] - mean)
    variance = inside * (1.0 / (rows * py)) + between * (1.0 / py)
    mean_out[...] = mean
    scale_out[...] = lax.rsqrt(variance + 0.0001)
    for copy in sums:
        copy.wait_send()

CHUNKS = 4


def finish(density, mean, scale, anomaly_out, density_out, anomaly, sem):
    rows = density.shape[0]
    whole = pltpu.make_async_copy(density, density_out, sem.at[CHUNKS])
    whole.start()
    part = rows // CHUNKS
    copies = []
    for chunk in range(CHUNKS):
        for i in range(chunk * part, (chunk + 1) * part):
            anomaly[i] = (density[i] - mean[...]) * scale[...]
        own = pl.ds(chunk * part, part)
        copies.append(pltpu.make_async_copy(anomaly.at[own], anomaly_out.at[own], sem.at[chunk]))
        copies[-1].start()
    for copy in copies:
        copy.wait()
    whole.wait()


def per_device(py, px, inner, density, conductance, source):
    rows, columns, levels = density.shape
    tall, width = rows + 2 * DEEP, columns + 2 * PAD
    vmem = pl.BlockSpec(memory_space=pltpu.VMEM)
    line = jax.ShapeDtypeStruct((columns, levels), jnp.float32)
    density, conductance, source = (pltpu.with_memory_space_constraint(x, pltpu.HBM) for x in (density, conductance, source))
    density, mean, scale = pl.pallas_call(
        functools.partial(kernel, py, px, inner),
        out_shape=[jax.ShapeDtypeStruct(density.shape, jnp.float32), line, line],
        in_specs=[pl.BlockSpec(memory_space=pltpu.HBM)] * 3,
        out_specs=[vmem] * 3,
        scratch_shapes=[
            pltpu.VMEM((len(ROUNDS), tall, width, levels), jnp.float32),
            pltpu.VMEM((DEEP - 1, tall, width, levels), jnp.float32),
            pltpu.VMEM((2, tall, width, levels), jnp.float32),
            pltpu.VMEM((py, 2, columns, levels), jnp.float32),
            pltpu.SemaphoreType.DMA((3,)),
            pltpu.SemaphoreType.DMA((len(ROUNDS), 3, len(DIRECTIONS))),
            pltpu.SemaphoreType.DMA((len(ROUNDS), 3, len(DIRECTIONS))),
            pltpu.SemaphoreType.DMA((py,)),
            pltpu.SemaphoreType.DMA((py,)),
        ],
        compiler_params=pltpu.CompilerParams(collective_id=0, has_side_effects=True, vmem_limit_bytes=10*2**20),
    )(density, conductance, source)
    return pl.pallas_call(
        finish,
        out_shape=[jax.ShapeDtypeStruct(density.shape, jnp.float32)] * 2,
        in_specs=[vmem] * 3,
        out_specs=[pl.BlockSpec(memory_space=pltpu.HBM)] * 2,
        scratch_shapes=[pltpu.VMEM(density.shape, jnp.float32), pltpu.SemaphoreType.DMA((CHUNKS + 1,))],
        compiler_params=pltpu.CompilerParams(vmem_limit_bytes=4 * 2**20),
    )(density, mean, scale)


def solution(mesh):
    spec = P("py", "px", None)
    line = mesh.devices.reshape(mesh.shape["py"], -1)[:, 0] if mesh.axis_names[0] == "py" else []
    places = [getattr(device, "coords", (0, 0, 0))[2] for device in line]
    inner = max(1, places.count(places[0])) if places else 1
    return jax.shard_map(
        functools.partial(per_device, mesh.shape["py"], mesh.shape["px"], inner),
        mesh=mesh, in_specs=(spec,) * 3, out_specs=(spec,) * 2, check_vma=False,
    )
```

```python
import functools

import jax
import jax.numpy as jnp
from jax import lax
from jax.experimental import pallas as pl
from jax.experimental.pallas import tpu as pltpu
from jax.sharding import PartitionSpec as P

ROUNDS = (3, 3)
DEEP = max(ROUNDS)
PAD = 4
DIRECTIONS = [(-1, -1), (-1, 1), (1, -1), (1, 1), (-1, 0), (1, 0), (0, -1), (0, 1)]
MESH = pl.DeviceIdType.MESH


def edge(direction, size, depth, own):
    if direction < 0:
        return (own, depth), (own + size, depth)
    if direction > 0:
        return (own + size - depth, depth), (own - depth, depth)
    return (own, size), (own, size)


def kernel(py, px, inner, field, conductance, source, density_out, mean_out, scale_out,
           padded, work, coefficients, stats, local_sem, send_sem, recv_sem, stat_send, stat_recv):
    rows, columns, levels = field.shape
    width = columns + 2 * PAD
    my, mx = lax.axis_index("py"), lax.axis_index("px")

    def exists(dy, dx):
        here = jnp.bool_(True)
        if dy:
            here = here & ((my > 0) if dy < 0 else (my < py - 1))
        if dx:
            here = here & ((mx > 0) if dx < 0 else (mx < px - 1))
        return here

    block = (pl.ds(DEEP, rows), pl.ds(PAD, columns))
    loads = []
    for i, (src, dst) in enumerate(
        [(field, padded.at[0]), (conductance, coefficients.at[0]), (source, coefficients.at[1])]
    ):
        loads.append(pltpu.make_async_copy(src, dst.at[block], local_sem.at[i]))
        loads[-1].start()

    barrier = pltpu.get_barrier_semaphore()
    expected = jnp.int32(py - 1)
    for step in range(1, py):
        pl.semaphore_signal(barrier, 1, device_id=(lax.rem(my + step, py), mx), device_id_type=MESH)
    for dy, dx in DIRECTIONS:
        if dx:
            there = exists(dy, dx)
            expected = expected + there.astype(jnp.int32)

            @pl.when(there)
            def _():
                pl.semaphore_signal(barrier, 1, device_id=(my + dy, mx + dx), device_id_type=MESH)

    holders = [padded.at[r] for r in range(len(ROUNDS))] + [coefficients.at[0], coefficients.at[1]]
    for dim, direction in ((0, -1), (0, 1), (1, -1), (1, 1)):
        outside = ~exists(*((direction, 0) if dim == 0 else (0, direction)))

        @pl.when(outside)
        def _():
            for holder in holders:
                if dim == 0:
                    start = 0 if direction < 0 else DEEP + rows
                    holder[pl.ds(start, DEEP)] = jnp.zeros((DEEP, width, levels), jnp.float32)
                else:
                    start = 0 if direction < 0 else PAD + columns
                    holder[:, pl.ds(start, PAD)] = jnp.zeros((rows + 2 * DEEP, PAD, levels), jnp.float32)

    pl.semaphore_wait(barrier, expected)

    def exchange(number, arrays):
        for d, (dy, dx) in enumerate(DIRECTIONS):
            copies = []
            for a, (src, row0, column0, dst, depth) in enumerate(arrays):
                reach = depth - 1 if dy and dx else depth
                if reach < 1:
                    continue
                (y_from, y_size), _ = edge(dy, rows, reach, row0)
                (x_from, x_size), _ = edge(dx, columns, reach, column0)
                _, (y_to, _) = edge(dy, rows, reach, DEEP)
                _, (x_to, _) = edge(dx, columns, reach, PAD)
                both = (slice(None),) * (len(src.shape) - 3)
                copies.append(
                    pltpu.make_async_remote_copy(
                        src_ref=src.at[both + (pl.ds(y_from, y_size), pl.ds(x_from, x_size))],
                        dst_ref=dst.at[both + (pl.ds(y_to, y_size), pl.ds(x_to, x_size))],
                        send_sem=send_sem.at[number, a, d],
                        recv_sem=recv_sem.at[number, a, d],
                        device_id=(my + dy, mx + dx),
                        device_id_type=MESH,
                    )
                )
            yield (dy, dx), copies

    def start(copies):
        for (dy, dx), group in copies:
            @pl.when(exists(dy, dx))
            def _():
                for copy in group:
                    copy.start()

    def wait_recv(copies):
        for (dy, dx), group in copies:
            @pl.when(exists(-dy, -dx))
            def _():
                for copy in group:
                    copy.wait_recv()

    def wait_send(copies):
        for (dy, dx), group in copies:
            @pl.when(exists(dy, dx))
            def _():
                for copy in group:
                    copy.wait_send()

    tall = rows + 2 * DEEP
    flat_conductance = coefficients.at[0].reshape(tall * width, levels)
    flat_source = coefficients.at[1].reshape(tall * width, levels)

    def advance(old, first, count, column, wide, put, carry):
        flat = old.reshape(tall * width, levels)

        def row(i, state):
            above, middle, carry = state
            at = (first + i) * width + column
            below = flat[pl.ds(at + width, wide), :]
            sides = flat[pl.ds(at - 1, wide), :] + flat[pl.ds(at + 1, wide), :]
            spread = (above + below) + sides - 4.0 * middle
            later = middle + flat_conductance[pl.ds(at, wide), :] * spread + flat_source[pl.ds(at, wide), :]
            return middle, below, put(first - DEEP + i, later, carry)

        at = first * width + column
        state = (flat[pl.ds(at - width, wide), :], flat[pl.ds(at, wide), :], carry)
        return lax.fori_loop(0, count, row, state, unroll=min(count, 4))[2]

    total = jnp.zeros((columns, levels), jnp.float32)
    waiting = []
    for number, steps in enumerate(ROUNDS):
        if number == 0:
            arrays = [
                (padded.at[0], DEEP, PAD, padded.at[0], steps),
                (coefficients, DEEP, PAD, coefficients, DEEP - 1),
            ]
        else:
            arrays = [(padded.at[number], DEEP, PAD, padded.at[number], steps)]
        copies = list(exchange(number, arrays))
        if number == 0:
            for copy in loads:
                copy.wait()
        start(copies)
        waiting.append(copies)
        across = [copy for copy in copies if not copy[0][0]]
        wait_recv(across)
        for part in ("inside", "low", "high"):
            if part != "inside":
                sent = 1 if part == "low" else -1
                wait_recv([copy for copy in copies if copy[0][0] == sent])
            old = padded.at[number]
            for step in range(steps):
                margin = steps - 1 - step
                if part == "inside":
                    spans = [(DEEP + step + 1, rows - 2 * (step + 1))]
                elif part == "low":
                    spans = [(DEEP - margin, steps)]
                else:
                    spans = [(DEEP + rows - step - 1, steps)]
                column, wide, new = PAD, columns, None
                if margin:
                    column, wide, new = 0, width, work.at[step]
                elif number < len(ROUNDS) - 1:
                    new = padded.at[number + 1]

                def put(i, later, carry, new=new, column=column, wide=wide):
                    if new is None:
                        density_out[i] = later
                        return carry + later
                    new.reshape(tall * width, levels)[pl.ds((DEEP + i) * width + column, wide), :] = later
                    return carry

                for first, count in spans:
                    total = advance(old, first, count, column, wide, put, total)
                old = new

    local_mean = total * (1.0 / rows)

    def square(i, carry):
        away = density_out[i] - local_mean
        return carry + away * away

    squares = lax.fori_loop(0, rows, square, jnp.zeros((columns, levels), jnp.float32), unroll=4)
    stats[0, 0] = local_mean
    stats[0, 1] = squares
    outer = py // inner
    far_first = sorted(
        ((do, di) for do in range(outer) for di in range(inner) if do or di),
        key=lambda place: -(min(place[0], outer - place[0]) + min(place[1], inner - place[1])),
    )
    sums = []
    for do, di in far_first:
        step = do * inner + di
        peer = lax.rem(my // inner + do, outer) * inner + lax.rem(lax.rem(my, inner) + di, inner)
        copy = pltpu.make_async_remote_copy(
            src_ref=stats.at[0],
            dst_ref=stats.at[step],
            send_sem=stat_send.at[step],
            recv_sem=stat_recv.at[step],
            device_id=(peer, mx),
            device_id_type=MESH,
        )
        copy.start()
        sums.append(copy)
    for copies in waiting:
        wait_send(copies)
    for copy in sums:
        copy.wait_recv()
    mean = stats[0, 0]
    for step in range(1, py):
        mean = mean + stats[step, 0]
    mean = mean * (1.0 / py)
    inside = stats[0, 1]
    between = (stats[0, 0] - mean) * (stats[0, 0] - mean)
    for step in range(1, py):
        inside = inside + stats[step, 1]
        between = between + (stats[step, 0] - mean) * (stats[step, 0] - mean)
    variance = inside * (1.0 / (rows * py)) + between * (1.0 / py)
    mean_out[...] = mean
    scale_out[...] = lax.rsqrt(variance + 0.0001)
    for copy in sums:
        copy.wait_send()

CHUNKS = 2


def finish(density, mean, scale, anomaly_out, density_out, anomaly, sem):
    rows = density.shape[0]
    whole = pltpu.make_async_copy(density, density_out, sem.at[CHUNKS])
    whole.start()
    part = rows // CHUNKS
    copies = []
    for chunk in range(CHUNKS):
        for i in range(chunk * part, (chunk + 1) * part):
            anomaly[i] = (density[i] - mean[...]) * scale[...]
        own = pl.ds(chunk * part, part)
        copies.append(pltpu.make_async_copy(anomaly.at[own], anomaly_out.at[own], sem.at[chunk]))
        copies[-1].start()
    for copy in copies:
        copy.wait()
    whole.wait()


def per_device(py, px, inner, density, conductance, source):
    rows, columns, levels = density.shape
    tall, width = rows + 2 * DEEP, columns + 2 * PAD
    vmem = pl.BlockSpec(memory_space=pltpu.VMEM)
    line = jax.ShapeDtypeStruct((columns, levels), jnp.float32)
    density, conductance, source = (pltpu.with_memory_space_constraint(x, pltpu.HBM) for x in (density, conductance, source))
    density, mean, scale = pl.pallas_call(
        functools.partial(kernel, py, px, inner),
        out_shape=[jax.ShapeDtypeStruct(density.shape, jnp.float32), line, line],
        in_specs=[pl.BlockSpec(memory_space=pltpu.HBM)] * 3,
        out_specs=[vmem] * 3,
        scratch_shapes=[
            pltpu.VMEM((len(ROUNDS), tall, width, levels), jnp.float32),
            pltpu.VMEM((DEEP - 1, tall, width, levels), jnp.float32),
            pltpu.VMEM((2, tall, width, levels), jnp.float32),
            pltpu.VMEM((py, 2, columns, levels), jnp.float32),
            pltpu.SemaphoreType.DMA((3,)),
            pltpu.SemaphoreType.DMA((len(ROUNDS), 3, len(DIRECTIONS))),
            pltpu.SemaphoreType.DMA((len(ROUNDS), 3, len(DIRECTIONS))),
            pltpu.SemaphoreType.DMA((py,)),
            pltpu.SemaphoreType.DMA((py,)),
        ],
        compiler_params=pltpu.CompilerParams(collective_id=0, has_side_effects=True, vmem_limit_bytes=10*2**20),
    )(density, conductance, source)
    return pl.pallas_call(
        finish,
        out_shape=[jax.ShapeDtypeStruct(density.shape, jnp.float32)] * 2,
        in_specs=[vmem] * 3,
        out_specs=[pl.BlockSpec(memory_space=pltpu.HBM)] * 2,
        scratch_shapes=[pltpu.VMEM(density.shape, jnp.float32), pltpu.SemaphoreType.DMA((CHUNKS + 1,))],
        compiler_params=pltpu.CompilerParams(vmem_limit_bytes=4 * 2**20),
    )(density, mean, scale)


def solution(mesh):
    spec = P("py", "px", None)
    line = mesh.devices.reshape(mesh.shape["py"], -1)[:, 0] if mesh.axis_names[0] == "py" else []
    places = [getattr(device, "coords", (0, 0, 0))[2] for device in line]
    inner = max(1, places.count(places[0])) if places else 1
    return jax.shard_map(
        functools.partial(per_device, mesh.shape["py"], mesh.shape["px"], inner),
        mesh=mesh, in_specs=(spec,) * 3, out_specs=(spec,) * 2, check_vma=False,
    )
```

```python
import functools

import jax
import jax.numpy as jnp
from jax import lax
from jax.experimental import pallas as pl
from jax.experimental.pallas import tpu as pltpu
from jax.sharding import PartitionSpec as P

ROUNDS = (3, 3)
DEEP = max(ROUNDS)
PAD = 4
DIRECTIONS = [(-1, -1), (-1, 1), (1, -1), (1, 1), (-1, 0), (1, 0), (0, -1), (0, 1)]
MESH = pl.DeviceIdType.MESH


def edge(direction, size, depth, own):
    if direction < 0:
        return (own, depth), (own + size, depth)
    if direction > 0:
        return (own + size - depth, depth), (own - depth, depth)
    return (own, size), (own, size)


def kernel(py, px, inner, field, conductance, source, density_out, mean_out, scale_out,
           padded, work, coefficients, stats, local_sem, send_sem, recv_sem, stat_send, stat_recv):
    rows, columns, levels = field.shape
    width = columns + 2 * PAD
    my, mx = lax.axis_index("py"), lax.axis_index("px")

    def exists(dy, dx):
        here = jnp.bool_(True)
        if dy:
            here = here & ((my > 0) if dy < 0 else (my < py - 1))
        if dx:
            here = here & ((mx > 0) if dx < 0 else (mx < px - 1))
        return here

    barrier = pltpu.get_barrier_semaphore()
    expected = jnp.int32(py - 1)
    for step in range(1, py):
        pl.semaphore_signal(barrier, 1, device_id=(lax.rem(my + step, py), mx), device_id_type=MESH)
    for dy, dx in DIRECTIONS:
        if dx:
            there = exists(dy, dx)
            expected = expected + there.astype(jnp.int32)

            @pl.when(there)
            def _():
                pl.semaphore_signal(barrier, 1, device_id=(my + dy, mx + dx), device_id_type=MESH)

    block = (pl.ds(DEEP, rows), pl.ds(PAD, columns))
    loads = []
    for i, (src, dst) in enumerate(
        [(field, padded.at[0]), (conductance, coefficients.at[0]), (source, coefficients.at[1])]
    ):
        loads.append(pltpu.make_async_copy(src, dst.at[block], local_sem.at[i]))
        loads[-1].start()

    holders = [padded.at[r] for r in range(len(ROUNDS))] + [coefficients.at[0], coefficients.at[1]]
    for dim, direction in ((0, -1), (0, 1), (1, -1), (1, 1)):
        outside = ~exists(*((direction, 0) if dim == 0 else (0, direction)))

        @pl.when(outside)
        def _():
            for holder in holders:
                if dim == 0:
                    start = 0 if direction < 0 else DEEP + rows
                    holder[pl.ds(start, DEEP)] = jnp.zeros((DEEP, width, levels), jnp.float32)
                else:
                    start = 0 if direction < 0 else PAD + columns
                    holder[:, pl.ds(start, PAD)] = jnp.zeros((rows + 2 * DEEP, PAD, levels), jnp.float32)

    pl.semaphore_wait(barrier, expected)

    def exchange(number, arrays):
        for d, (dy, dx) in enumerate(DIRECTIONS):
            copies = []
            for a, (src, row0, column0, dst, depth) in enumerate(arrays):
                reach = depth - 1 if dy and dx else depth
                if reach < 1:
                    continue
                (y_from, y_size), _ = edge(dy, rows, reach, row0)
                (x_from, x_size), _ = edge(dx, columns, reach, column0)
                _, (y_to, _) = edge(dy, rows, reach, DEEP)
                _, (x_to, _) = edge(dx, columns, reach, PAD)
                copies.append(
                    pltpu.make_async_remote_copy(
                        src_ref=src.at[pl.ds(y_from, y_size), pl.ds(x_from, x_size)],
                        dst_ref=dst.at[pl.ds(y_to, y_size), pl.ds(x_to, x_size)],
                        send_sem=send_sem.at[number, a, d],
                        recv_sem=recv_sem.at[number, a, d],
                        device_id=(my + dy, mx + dx),
                        device_id_type=MESH,
                    )
                )
            yield (dy, dx), copies

    def start(copies):
        for (dy, dx), group in copies:
            @pl.when(exists(dy, dx))
            def _():
                for copy in group:
                    copy.start()

    def wait_recv(copies):
        for (dy, dx), group in copies:
            @pl.when(exists(-dy, -dx))
            def _():
                for copy in group:
                    copy.wait_recv()

    def wait_send(copies):
        for (dy, dx), group in copies:
            @pl.when(exists(dy, dx))
            def _():
                for copy in group:
                    copy.wait_send()

    tall = rows + 2 * DEEP
    flat_conductance = coefficients.at[0].reshape(tall * width, levels)
    flat_source = coefficients.at[1].reshape(tall * width, levels)

    def advance(old, first, count, column, wide, put, carry):
        flat = old.reshape(tall * width, levels)

        def row(i, state):
            above, middle, carry = state
            at = (first + i) * width + column
            below = flat[pl.ds(at + width, wide), :]
            sides = flat[pl.ds(at - 1, wide), :] + flat[pl.ds(at + 1, wide), :]
            spread = (above + below) + sides - 4.0 * middle
            later = middle + flat_conductance[pl.ds(at, wide), :] * spread + flat_source[pl.ds(at, wide), :]
            return middle, below, put(first - DEEP + i, later, carry)

        at = first * width + column
        state = (flat[pl.ds(at - width, wide), :], flat[pl.ds(at, wide), :], carry)
        return lax.fori_loop(0, count, row, state, unroll=min(count, 4))[2]

    total = jnp.zeros((columns, levels), jnp.float32)
    waiting = []
    for number, steps in enumerate(ROUNDS):
        if number == 0:
            arrays = [
                (padded.at[0], DEEP, PAD, padded.at[0], steps),
                (coefficients.at[0], DEEP, PAD, coefficients.at[0], DEEP - 1),
                (coefficients.at[1], DEEP, PAD, coefficients.at[1], DEEP - 1),
            ]
        else:
            arrays = [(padded.at[number], DEEP, PAD, padded.at[number], steps)]
        copies = list(exchange(number, arrays))
        if number == 0:
            for copy in loads:
                copy.wait()
        start(copies)
        waiting.append(copies)
        across = [copy for copy in copies if not copy[0][0]]
        wait_recv(across)
        for part in ("inside", "ends"):
            if part == "ends":
                wait_recv([copy for copy in copies if copy[0][0]])
            old = padded.at[number]
            for step in range(steps):
                margin = steps - 1 - step
                if part == "inside":
                    spans = [(DEEP + step + 1, rows - 2 * (step + 1))]
                else:
                    spans = [(DEEP - margin, steps), (DEEP + rows - step - 1, steps)]
                column, wide, new = PAD, columns, None
                if margin:
                    column, wide, new = 0, width, work.at[step]
                elif number < len(ROUNDS) - 1:
                    new = padded.at[number + 1]

                def put(i, later, carry, new=new, column=column, wide=wide):
                    if new is None:
                        density_out[i] = later
                        return carry + later
                    new.reshape(tall * width, levels)[pl.ds((DEEP + i) * width + column, wide), :] = later
                    return carry

                for first, count in spans:
                    total = advance(old, first, count, column, wide, put, total)
                old = new

    local_mean = total * (1.0 / rows)

    def square(i, carry):
        away = density_out[i] - local_mean
        return carry + away * away

    squares = lax.fori_loop(0, rows, square, jnp.zeros((columns, levels), jnp.float32), unroll=4)
    stats[0, 0] = local_mean
    stats[0, 1] = squares
    outer = py // inner
    far_first = sorted(
        ((do, di) for do in range(outer) for di in range(inner) if do or di),
        key=lambda place: (-min(place[0], outer - place[0]), -place[1]),
    )
    sums = []
    for do, di in far_first:
        step = do * inner + di
        peer = lax.rem(my // inner + do, outer) * inner + lax.rem(lax.rem(my, inner) + di, inner)
        copy = pltpu.make_async_remote_copy(
            src_ref=stats.at[0],
            dst_ref=stats.at[step],
            send_sem=stat_send.at[step],
            recv_sem=stat_recv.at[step],
            device_id=(peer, mx),
            device_id_type=MESH,
        )
        copy.start()
        sums.append(copy)
    for copies in waiting:
        wait_send(copies)
    for copy in sums:
        copy.wait_recv()
    mean = stats[0, 0]
    for step in range(1, py):
        mean = mean + stats[step, 0]
    mean = mean * (1.0 / py)
    inside = stats[0, 1]
    between = (stats[0, 0] - mean) * (stats[0, 0] - mean)
    for step in range(1, py):
        inside = inside + stats[step, 1]
        between = between + (stats[step, 0] - mean) * (stats[step, 0] - mean)
    variance = inside * (1.0 / (rows * py)) + between * (1.0 / py)
    mean_out[...] = mean
    scale_out[...] = lax.rsqrt(variance + 0.0001)
    for copy in sums:
        copy.wait_send()

CHUNKS = 4


def finish(density, mean, scale, anomaly_out, density_out, anomaly, sem):
    rows = density.shape[0]
    whole = pltpu.make_async_copy(density, density_out, sem.at[CHUNKS])
    whole.start()
    part = rows // CHUNKS
    copies = []
    for chunk in range(CHUNKS):
        for i in range(chunk * part, (chunk + 1) * part):
            anomaly[i] = (density[i] - mean[...]) * scale[...]
        own = pl.ds(chunk * part, part)
        copies.append(pltpu.make_async_copy(anomaly.at[own], anomaly_out.at[own], sem.at[chunk]))
        copies[-1].start()
    for copy in copies:
        copy.wait()
    whole.wait()


def per_device(py, px, inner, density, conductance, source):
    rows, columns, levels = density.shape
    tall, width = rows + 2 * DEEP, columns + 2 * PAD
    vmem = pl.BlockSpec(memory_space=pltpu.VMEM)
    line = jax.ShapeDtypeStruct((columns, levels), jnp.float32)
    density, conductance, source = (pltpu.with_memory_space_constraint(x, pltpu.HBM) for x in (density, conductance, source))
    density, mean, scale = pl.pallas_call(
        functools.partial(kernel, py, px, inner),
        out_shape=[jax.ShapeDtypeStruct(density.shape, jnp.float32), line, line],
        in_specs=[pl.BlockSpec(memory_space=pltpu.HBM)] * 3,
        out_specs=[vmem] * 3,
        scratch_shapes=[
            pltpu.VMEM((len(ROUNDS), tall, width, levels), jnp.float32),
            pltpu.VMEM((DEEP - 1, tall, width, levels), jnp.float32),
            pltpu.VMEM((2, tall, width, levels), jnp.float32),
            pltpu.VMEM((py, 2, columns, levels), jnp.float32),
            pltpu.SemaphoreType.DMA((3,)),
            pltpu.SemaphoreType.DMA((len(ROUNDS), 3, len(DIRECTIONS))),
            pltpu.SemaphoreType.DMA((len(ROUNDS), 3, len(DIRECTIONS))),
            pltpu.SemaphoreType.DMA((py,)),
            pltpu.SemaphoreType.DMA((py,)),
        ],
        compiler_params=pltpu.CompilerParams(collective_id=0, has_side_effects=True, vmem_limit_bytes=10*2**20),
    )(density, conductance, source)
    return pl.pallas_call(
        finish,
        out_shape=[jax.ShapeDtypeStruct(density.shape, jnp.float32)] * 2,
        in_specs=[vmem] * 3,
        out_specs=[pl.BlockSpec(memory_space=pltpu.HBM)] * 2,
        scratch_shapes=[pltpu.VMEM(density.shape, jnp.float32), pltpu.SemaphoreType.DMA((CHUNKS + 1,))],
        compiler_params=pltpu.CompilerParams(vmem_limit_bytes=4 * 2**20),
    )(density, mean, scale)


def solution(mesh):
    spec = P("py", "px", None)
    line = mesh.devices.reshape(mesh.shape["py"], -1)[:, 0] if mesh.axis_names[0] == "py" else []
    places = [getattr(device, "coords", (0, 0, 0))[2] for device in line]
    inner = max(1, places.count(places[0])) if places else 1
    return jax.shard_map(
        functools.partial(per_device, mesh.shape["py"], mesh.shape["px"], inner),
        mesh=mesh, in_specs=(spec,) * 3, out_specs=(spec,) * 2, check_vma=False,
    )
```
